32 devices in a mesh: rep: 1, r: 8 (over y, z), s: 4 (over x, core).
Axes of the slice: x: 2, y: 2, z: 4, core: 2. Of those that a mesh axis runs over, the one named last changes fastest.
Arguments:
- x: bfloat16 [32, 4096, 640], P(('rep', 'r', 's'))
- dy: bfloat16 [32, 4096, 640], P(('rep', 'r', 's'))
- w_gate: bfloat16 [2, 640, 2560], P(None, 's')
- w_up: bfloat16 [2, 640, 2560], P(None, 's')
- w_down: bfloat16 [2, 2560, 640], P(None, 's')
Outputs:
- output 1: bfloat16 [32, 4096, 640], P(('rep', 'r', 's'))
- output 2: bfloat16 [2, 640, 2560], P('rep', 's')
- output 3: bfloat16 [2, 640, 2560], P('rep', 's')
- output 4: bfloat16 [2, 2560, 640], P('rep', 's')
All inputs are finite; a program needn't handle non-finite values.
Results may differ from the reference program's by a relative error of at most 0.018.
Values are sent between devices in bfloat16 or wider.
A program may use at most 2 GiB of HBM per device.

```python
import jax
import jax.numpy as jnp
from jax import lax

SEQUENCES = 32
TOKENS = 4096
D = 640
FF = 2560
LAYERS = 2
NAMES = ("w_gate", "w_up", "w_down")
SHAPES = {"w_gate": (LAYERS, D, FF), "w_up": (LAYERS, D, FF), "w_down": (LAYERS, FF, D)}


def bump(key, n, height):
    away = (jnp.arange(n, dtype=jnp.int32) - jax.random.randint(key, (), 0, n, jnp.int32)) % n
    return jnp.where(away < n // 8, height, 1.0)


def together(key, own, strength):
    shared = jax.random.normal(key, own.shape[1:], jnp.float32)
    return (own + strength * shared) * lax.rsqrt(1 + strength * strength)


def setup_inputs(seed: int = 0, part: int = 0) -> dict:
    kx, kdy, ka, kb, kz, kf, kh, kl, *kw = jax.random.split(jax.random.key(seed), 8 + len(NAMES))
    kx, kdy, ka, kb = (jax.random.fold_in(k, part) for k in (kx, kdy, ka, kb))
    shape = (SEQUENCES, TOKENS, D)
    much_x, much_dy = jax.random.uniform(kz, (2,), jnp.float32, 0.0, 1.0)
    layers = 2.0 ** jax.random.uniform(kl, (LAYERS, 1, 1), jnp.float32, -1.0, 1.0)
    x = together(ka, jax.random.normal(kx, shape, jnp.float32), much_x) * bump(kf, D, 4.0)
    dy = together(kb, jax.random.normal(kdy, shape, jnp.float32), much_dy)
    drawn = {"x": x.astype(jnp.bfloat16), "dy": (dy * (SEQUENCES * TOKENS) ** -0.5).astype(jnp.bfloat16)}
    for key, name in zip(kw, NAMES, strict=True):
        w = jax.random.normal(key, SHAPES[name], jnp.float32) * SHAPES[name][1] ** -0.5
        drawn[name] = (w * {"w_gate": 1.0, "w_up": bump(kh, FF, 4.0), "w_down": layers}[name]).astype(jnp.bfloat16)
    return drawn


def matmul(a, w):
    return jnp.dot(a, w, preferred_element_type=jnp.float32).astype(jnp.bfloat16)


def normed(h):
    wide = h.astype(jnp.float32)
    scale = lax.rsqrt(jnp.mean(wide**2, -1, keepdims=True) + 1e-6)
    return (wide * scale).astype(jnp.bfloat16)


def layer(h, w):
    a = normed(h)
    gate = jnp.dot(a, w["w_gate"], preferred_element_type=jnp.float32)
    up = jnp.dot(a, w["w_up"], preferred_element_type=jnp.float32)
    return h + matmul((jax.nn.silu(gate) * up).astype(jnp.bfloat16), w["w_down"])


def stack(weights, h):
    return lax.scan(lambda h, w: (layer(h, w), None), h, weights)[0]


def reference(x, dy, w_gate, w_up, w_down):
    weights = dict(zip(NAMES, (w_gate, w_up, w_down), strict=True))

    def take(so_far, sequence):
        h, by_y = sequence
        _, back = jax.vjp(stack, weights, h)
        by_weights, by_h = back(by_y)
        return jax.tree.map(lambda total, term: total + term.astype(jnp.float32), so_far, by_weights), by_h

    none_yet = {name: jnp.zeros(w.shape, jnp.float32) for name, w in weights.items()}
    by_weights, by_x = lax.scan(take, none_yet, (x, dy))
    return (by_x, *(by_weights[name].astype(jnp.bfloat16) for name in NAMES))
```

```python
import functools

import jax
import jax.numpy as jnp
from jax import lax
from jax.experimental import pallas as pl
from jax.experimental.pallas import tpu as pltpu
from jax.sharding import PartitionSpec as P

T, D, FF = 4096, 640, 2560
R = 512
NR = T // R
F, C = 5, 512
Q = 2 * F
NS, NG = 4, 8
PIECE = 240
BF, F32 = jnp.bfloat16, jnp.float32
MB = 1 << 20
NT = (((1,), (1,)), ((), ()))


def dot(a, b):
    return jnp.dot(a, b, preferred_element_type=F32)


def dot_nt(a, b):
    return lax.dot_general(a, b, NT, preferred_element_type=F32)


def sigmoid(v):
    return 1.0 / (1.0 + jnp.exp(-v))


def scale_of(wide):
    return lax.rsqrt(jnp.mean(wide * wide, -1, keepdims=True) + 1e-6)


def forward_kernel(x_ref, wg_ref, wu_ref, wd_ref, h_ref, prod_ref):
    wide = x_ref[...].astype(F32)
    a = (wide * scale_of(wide)).astype(BF)
    for f in range(F):
        cols = pl.ds(f * C, C)
        gate = dot(a, wg_ref[:, cols])
        up = dot(a, wu_ref[:, cols])
        prod_ref[:, cols] = (gate * sigmoid(gate) * up).astype(BF)
    h_ref[...] = (wide + dot(prod_ref[...], wd_ref[...]).astype(BF).astype(F32)).astype(BF)


def forward(x, wg, wu, wd):
    whole = lambda shape: pl.BlockSpec(shape, lambda i: (0, 0), pipeline_mode=pl.Buffered(1))
    return pl.pallas_call(
        forward_kernel,
        grid=(NR,),
        in_specs=[pl.BlockSpec((R, D), lambda i: (i, 0)), whole((D, FF)), whole((D, FF)), whole((FF, D))],
        out_specs=pl.BlockSpec((R, D), lambda i: (i, 0)),
        out_shape=jax.ShapeDtypeStruct((T, D), BF),
        scratch_shapes=[pltpu.VMEM((R, FF), BF)],
        compiler_params=pltpu.CompilerParams(vmem_limit_bytes=50 * MB),
        cost_estimate=pl.CostEstimate(flops=6 * T * D * FF, bytes_accessed=20 * MB, transcendentals=0),
        name="forward",
    )(x, wg, wu, wd)


def backward_kernel(h1_ref, x_ref, dy_hbm, wg1, wu1, wd1, wg0, wu0, wd0,
                    dx_ref, out_hbm, ra_hbm, rb_hbm,
                    a_s, at_s, dy_s, dyt_s, da_s, accg, accu, accd, wg_s, wu_s, wd_s,
                    sa, sb, sc, va, vb,
                    w_sem, l_sem, sa_sem, ra_sem, sb_sem, rb_sem, sc_sem, rc_sem, own_sem):
    l, f, r = pl.program_id(0), pl.program_id(1), pl.program_id(2)
    q = l * F + f
    slot = lax.rem(q, 2)
    me_s, me_r = lax.axis_index("s"), lax.axis_index("r")
    rows = pl.ds(pl.multiple_of(r * R, R), R)

    def fetch(q, act):
        to = lax.rem(q, 2)
        fq = lax.rem(q, F)
        for layer, (wg, wu, wd) in enumerate(((wg1, wu1, wd1), (wg0, wu0, wd0))):
            @pl.when(q // F == layer)
            def _():
                for s in range(NS):
                    units = pl.ds(pl.multiple_of(640 * s + 128 * fq, 128), 128)
                    here = pl.ds(128 * s, 128)
                    act(pltpu.make_async_copy(wg.at[:, units], wg_s.at[to, :, here], w_sem.at[to, 0, s]))
                    act(pltpu.make_async_copy(wu.at[:, units], wu_s.at[to, :, here], w_sem.at[to, 1, s]))
                    act(pltpu.make_async_copy(wd.at[units], wd_s.at[to, here], w_sem.at[to, 2, s]))

    def a_copy(q, k):
        to = lax.rem(me_s + k, NS)
        return pltpu.make_async_remote_copy(sa.at[lax.rem(q, 2), to], ra_hbm.at[q, k - 1], sa_sem.at[lax.rem(q, 2), k - 1], ra_sem.at[q, k - 1],
                                            device_id={"s": to}, device_id_type=pl.DeviceIdType.MESH)

    def b_copy(q, k):
        to = lax.rem(me_r + k, NG)
        return pltpu.make_async_remote_copy(sb.at[lax.rem(q, 2), to], rb_hbm.at[q, k - 1], sb_sem.at[lax.rem(q, 2), k - 1], rb_sem.at[q, k - 1],
                                            device_id={"r": to}, device_id_type=pl.DeviceIdType.MESH)

    def c_copy(q, k):
        to = lax.rem(me_r + k, NG)
        return pltpu.make_async_remote_copy(sc.at[lax.rem(q, 2)], out_hbm.at[q, me_r], sc_sem.at[lax.rem(q, 2), k - 1], rc_sem.at[q, k - 1],
                                            device_id={"r": to}, device_id_type=pl.DeviceIdType.MESH)

    def own_copy(q):
        return pltpu.make_async_copy(sc.at[lax.rem(q, 2)], out_hbm.at[q, me_r], own_sem.at[lax.rem(q, 2)])

    def pack(q):
        to = lax.rem(q, 2)
        @pl.when(q >= 2)
        def _():
            for k in range(1, NS):
                a_copy(q - 2, k).wait_send()
        for s in range(NS):
            for j in range(NS):
                for b in range(6):
                    if b < 2:
                        v = accg[160 * s + 80 * b:160 * s + 80 * b + 80, 128 * j:128 * j + 128]
                    elif b < 4:
                        v = accu[160 * s + 80 * (b - 2):160 * s + 80 * (b - 2) + 80, 128 * j:128 * j + 128]
                    else:
                        v = accd[160 * j + 80 * (b - 4):160 * j + 80 * (b - 4) + 80, 128 * s:128 * s + 128]
                    at = 80 * (b % 3)
                    sa[to, s, 2 * j + b // 3, at:at + 80, :] = v.astype(BF)
        for k in range(1, NS):
            a_copy(q, k).start()

    def a_load(q):
        for k in range(1, NS):
            a_copy(q, k).wait_recv()
        pltpu.make_async_copy(ra_hbm.at[q], va, l_sem.at[0]).start()

    def a_add(q):
        to = lax.rem(q, 2)
        pltpu.make_async_copy(ra_hbm.at[q], va, l_sem.at[0]).wait()
        @pl.when(q >= 2)
        def _():
            for k in range(1, NG):
                b_copy(q - 2, k).wait_send()
        @pl.loop(0, NG)
        def _(p):
            total = sa[to, me_s, p].astype(F32)
            for k in range(NS - 1):
                total += va[k, p].astype(F32)
            sb[to, p] = total.astype(BF)
        for k in range(1, NG):
            b_copy(q, k).start()

    def b_load(q):
        for k in range(1, NG):
            b_copy(q, k).wait_recv()
        pltpu.make_async_copy(rb_hbm.at[q], vb, l_sem.at[1]).start()

    def b_add(q):
        to = lax.rem(q, 2)
        pltpu.make_async_copy(rb_hbm.at[q], vb, l_sem.at[1]).wait()
        @pl.when(q >= 2)
        def _():
            for k in range(1, NG):
                c_copy(q - 2, k).wait_send()
            own_copy(q - 2).wait()
        total = sb[to, me_r].astype(F32)
        for k in range(NG - 1):
            total += vb[k].astype(F32)
        sc[to] = total.astype(BF)
        own_copy(q).start()
        for k in range(1, NG):
            c_copy(q, k).start()

    @pl.when((q == 0) & (r == 0))
    def _():
        fetch(q, lambda c: c.start())
        whole_dy = pltpu.make_async_copy(dy_hbm, dy_s, l_sem.at[2])
        whole_dy.start()
        barrier = pltpu.get_barrier_semaphore()
        for k in range(1, NS):
            pl.semaphore_signal(barrier, inc=1, device_id={"s": lax.rem(me_s + k, NS)}, device_id_type=pl.DeviceIdType.MESH)
        for k in range(1, NG):
            pl.semaphore_signal(barrier, inc=1, device_id={"r": lax.rem(me_r + k, NG)}, device_id_type=pl.DeviceIdType.MESH)
        pl.semaphore_wait(barrier, NS + NG - 2)
        whole_dy.wait()

    @pl.when(r == 0)
    def _():
        fetch(q, lambda c: c.wait())
        accg[...] = jnp.zeros_like(accg)
        accu[...] = jnp.zeros_like(accu)
        accd[...] = jnp.zeros_like(accd)

    @pl.when((r == 1) & (q < Q - 1))
    def _():
        fetch(q + 1, lambda c: c.start())

    @pl.when(f == 0)
    def _():
        wide = jnp.where(l == 0, h1_ref[...], x_ref[...]).astype(F32)
        a = (wide * scale_of(wide)).astype(BF)
        a_s[rows] = a
        at_s[:, rows] = a.T
        da_s[rows] = jnp.zeros((R, D), F32)

    @pl.when(q == 0)
    def _():
        dyt_s[:, rows] = dy_s[rows].T

    a = a_s[rows]
    wg, wu, wd = wg_s[slot], wu_s[slot], wd_s[slot]
    gate = dot(a, wg)
    up = dot(a, wu)
    by_prod = dot_nt(dy_s[rows], wd).astype(BF).astype(F32)
    sig = sigmoid(gate)
    silu = gate * sig
    prod = (silu * up).astype(BF)
    by_up = (by_prod * silu).astype(BF)
    by_gate = (by_prod * up * (sig + silu * (1.0 - sig))).astype(BF)
    accd[...] += dot(dyt_s[:, rows], prod)
    at = at_s[:, rows]
    accg[...] += dot(at, by_gate)
    accu[...] += dot(at, by_up)
    da_s[rows] += dot_nt(by_gate, wg) + dot_nt(by_up, wu)

    @pl.when(f == F - 1)
    def _():
        wide = jnp.where(l == 0, h1_ref[...], x_ref[...]).astype(F32)
        scale = scale_of(wide)
        unit = wide * scale
        da = da_s[rows]
        by_wide = scale * (da - unit * jnp.mean(da * unit, -1, keepdims=True))
        by_h = (dy_s[rows].astype(F32) + by_wide.astype(BF).astype(F32)).astype(BF)
        dx_ref[...] = by_h
        dy_s[rows] = by_h
        dyt_s[:, rows] = by_h.T

    @pl.when((r == 6) & (q >= 1))
    def _():
        a_load(q - 1)

    @pl.when((r == 7) & (q >= 1))
    def _():
        a_add(q - 1)

    @pl.when(r == 7)
    def _():
        pack(q)

    @pl.when((r == 3) & (q >= 2))
    def _():
        b_load(q - 2)

    @pl.when((r == 4) & (q >= 2))
    def _():
        b_add(q - 2)

    @pl.when((q == Q - 1) & (r == NR - 1))
    def _():
        b_load(Q - 2)
        b_add(Q - 2)
        a_load(Q - 1)
        a_add(Q - 1)
        b_load(Q - 1)
        b_add(Q - 1)
        for last in (Q - 2, Q - 1):
            for k in range(1, NS):
                a_copy(last, k).wait_send()
            for k in range(1, NG):
                b_copy(last, k).wait_send()
                c_copy(last, k).wait_send()
            own_copy(last).wait()
        @pl.loop(0, Q)
        def _(each):
            for k in range(1, NG):
                c_copy(each, k).wait_recv()


def backward(h1, x, dy, w1, w0):
    hbm = pl.BlockSpec(memory_space=pl.ANY)

    def tile(layer):
        def at(l, f, r):
            here = (l == layer) & ((f == 0) | (f == F - 1))
            return jnp.where(here, r, jnp.where(l >= layer, NR - 1, 0)), 0
        return at

    def last(l, f, r):
        return jnp.where((l == 1) & (f == F - 1), r, 0), 0

    dma = pltpu.SemaphoreType.DMA
    dx, out, _, _ = pl.pallas_call(
        backward_kernel,
        grid=(2, F, NR),
        in_specs=[pl.BlockSpec((R, D), tile(0)), pl.BlockSpec((R, D), tile(1))] + [hbm] * 7,
        out_specs=[pl.BlockSpec((R, D), last), hbm, hbm, hbm],
        out_shape=[
            jax.ShapeDtypeStruct((T, D), BF),
            jax.ShapeDtypeStruct((Q, NG, PIECE, 128), BF),
            jax.ShapeDtypeStruct((Q, NS - 1, NG, PIECE, 128), BF),
            jax.ShapeDtypeStruct((Q, NG - 1, PIECE, 128), BF),
        ],
        scratch_shapes=[
            pltpu.VMEM((T, D), BF), pltpu.VMEM((D, T), BF), pltpu.VMEM((T, D), BF), pltpu.VMEM((D, T), BF),
            pltpu.VMEM((T, D), F32),
            pltpu.VMEM((D, C), F32), pltpu.VMEM((D, C), F32), pltpu.VMEM((D, C), F32),
            pltpu.VMEM((2, D, C), BF), pltpu.VMEM((2, D, C), BF), pltpu.VMEM((2, C, D), BF),
            pltpu.VMEM((2, NS, NG, PIECE, 128), BF), pltpu.VMEM((2, NG, PIECE, 128), BF), pltpu.VMEM((2, PIECE, 128), BF),
            pltpu.VMEM((NS - 1, NG, PIECE, 128), BF), pltpu.VMEM((NG - 1, PIECE, 128), BF),
            dma((2, 3, NS)), dma((3,)), dma((2, NS - 1)), dma((Q, NS - 1)), dma((2, NG - 1)), dma((Q, NG - 1)),
            dma((2, NG - 1)), dma((Q, NG - 1)), dma((2,)),
        ],
        compiler_params=pltpu.CompilerParams(
            dimension_semantics=("arbitrary",) * 3, vmem_limit_bytes=63 * MB, collective_id=1, has_side_effects=True),
        cost_estimate=pl.CostEstimate(flops=32 * T * D * FF, bytes_accessed=100 * MB, transcendentals=0),
        name="backward",
    )(h1, x, dy, *w1, *w0)
    return dx, out


def solution(mesh):
    def gathered(w):
        return lax.all_gather(w, "s", axis=0, tiled=True)

    def step(x, dy, *weights):
        w0 = [gathered(w[0]) for w in weights]
        h1 = forward(x[0], *w0)
        w1 = [gathered(w[1]) for w in weights]
        dx, out = backward(h1, x[0], dy[0], w1, w0)
        sums = out.reshape(2, F, NS, 480, 128)[::-1]
        cut = lambda i: sums[:, :, :, 160 * i:160 * (i + 1)]
        wide = lambda v: v.transpose(0, 3, 2, 1, 4).reshape(2, 160, FF)
        down = cut(2).transpose(0, 1, 4, 2, 3).reshape(2, D, D)
        return dx[None], wide(cut(0)), wide(cut(1)), down

    states, cut = P(("rep", "r", "s"), None, None), P(None, "s", None)
    return jax.shard_map(
        step,
        mesh=mesh,
        in_specs=(states, states) + (cut,) * 3,
        out_specs=(states,) + (P("rep", "s", None),) * 3,
        check_vma=False,
    )
```

```python
import functools

import jax
import jax.numpy as jnp
from jax import lax
from jax.experimental import pallas as pl
from jax.experimental.pallas import tpu as pltpu
from jax.sharding import PartitionSpec as P

T, D, FF = 4096, 640, 2560
R = 512
NR = T // R
F, C = 5, 512
Q = 2 * F
NS, NG = 4, 8
PIECE = 240
BF, F32 = jnp.bfloat16, jnp.float32
MB = 1 << 20
MESH = pl.DeviceIdType.MESH
NT = (((1,), (1,)), ((), ()))


def dot(a, b):
    return jnp.dot(a, b, preferred_element_type=F32)


def dot_nt(a, b):
    return lax.dot_general(a, b, NT, preferred_element_type=F32)


def sigmoid(v):
    return 1.0 / (1.0 + jnp.exp(-v))


def scale_of(wide):
    return lax.rsqrt(jnp.mean(wide * wide, -1, keepdims=True) + 1e-6)


def kernel(x_ref, dy_hbm, wg_in, wu_in, wd_in,
           dx_ref, out_hbm, ra_hbm, rb_hbm, h1_hbm, gg, gu, gd,
           a_s, at_s, dy_s, dyt_s, da_s, accg, accu, accd, wg_s, wu_s, wd_s,
           sa, sb, sc, va, vb, h_s,
           w_sem, l_sem, sa_sem, ra_sem, sb_sem, rb_sem, sc_sem, rc_sem, own_sem, h_sem, out_sem, in_sem):
    phase, f, r = pl.program_id(0), pl.program_id(1), pl.program_id(2)
    p = phase * F + f
    q = p - F
    slot = lax.rem(p, 2)
    me_s, me_r = lax.axis_index("s"), lax.axis_index("r")
    across = lax.rem(me_s + 2, NS)
    beside = me_s + 1 - 2 * lax.rem(me_s, 2)
    rows = pl.ds(pl.multiple_of(r * R, R), R)

    def mine(g):
        layer, part = g // F, lax.rem(g, F)
        for j in range(NS):
            units = pl.ds(pl.multiple_of(640 * j + 128 * part, 128), 128)
            yield 0, wg_in.at[layer, :, units], j
            yield 1, wu_in.at[layer, :, units], j
        yield 2, wd_in.at[layer, pl.ds(pl.multiple_of(128 * part, 128), 128)], 0

    def gather_send(g, way):
        to = across if way == 0 else beside
        owner = across if way == 2 else me_s
        if way == 2:
            pieces = [(m.at[g, owner], m.at[g, owner]) for m in (gg, gu, gd)]
        else:
            pieces = []
            for matrix, ref, j in mine(g):
                pieces.append((ref, gd.at[g, owner] if matrix == 2 else (gg, gu)[matrix].at[g, owner, :, pl.ds(128 * j, 128)]))
        for src, dst in pieces:
            pltpu.make_async_remote_copy(src, dst, out_sem.at[way, g], in_sem.at[way, g],
                                         device_id={"s": to}, device_id_type=MESH).start()

    def gather_wait(sem, g, way):
        pltpu.make_async_copy(ra_hbm.at[0, 0], ra_hbm.at[0, 0], sem.at[way, g]).wait()

    def relay(g):
        gather_wait(in_sem, g, 0)
        gather_send(g, 2)

    def fetch(p):
        to = lax.rem(p, 2)
        g = lax.rem(p, Q)
        for matrix, ref, j in mine(g):
            if matrix == 2:
                dst = wd_s.at[to, pl.ds(pl.multiple_of(128 * me_s, 128), 128)]
            else:
                dst = (wg_s, wu_s)[matrix].at[to, pl.ds(pl.multiple_of(160 * me_s, 32), 160), pl.ds(128 * j, 128)]
            pltpu.make_async_copy(ref, dst, w_sem.at[to, matrix]).start()
        for k in range(1, NS):
            s = lax.rem(me_s + k, NS)
            here = pl.ds(pl.multiple_of(160 * s, 32), 160)
            pltpu.make_async_copy(gg.at[g, s], wg_s.at[to, here], w_sem.at[to, 0]).start()
            pltpu.make_async_copy(gu.at[g, s], wu_s.at[to, here], w_sem.at[to, 1]).start()
            pltpu.make_async_copy(gd.at[g, s], wd_s.at[to, pl.ds(pl.multiple_of(128 * s, 128), 128)], w_sem.at[to, 2]).start()

    def fetched(p):
        to = lax.rem(p, 2)
        for matrix, w in enumerate((wg_s, wu_s, wd_s)):
            pltpu.make_async_copy(w.at[to], w.at[to], w_sem.at[to, matrix]).wait()

    def h_out(r):
        return pltpu.make_async_copy(h_s.at[lax.rem(r, 2)], h1_hbm.at[pl.ds(pl.multiple_of(r * R, R), R)], h_sem.at[lax.rem(r, 2)])

    def h_in(r):
        return pltpu.make_async_copy(h1_hbm.at[pl.ds(pl.multiple_of(r * R, R), R)], h_s.at[lax.rem(r, 2)], h_sem.at[lax.rem(r, 2)])


    def a_copy(q, k):
        to = lax.rem(me_s + k, NS)
        return pltpu.make_async_remote_copy(sa.at[lax.rem(q, 2), to], ra_hbm.at[q, k - 1], sa_sem.at[lax.rem(q, 2), k - 1], ra_sem.at[q, k - 1],
                                            device_id={"s": to}, device_id_type=MESH)

    def b_copy(q, k):
        to = lax.rem(me_r + k, NG)
        return pltpu.make_async_remote_copy(sb.at[lax.rem(q, 2), to], rb_hbm.at[q, k - 1], sb_sem.at[lax.rem(q, 2), k - 1], rb_sem.at[q, k - 1],
                                            device_id={"r": to}, device_id_type=MESH)

    def c_copy(q, k):
        to = lax.rem(me_r + k, NG)
        return pltpu.make_async_remote_copy(sc.at[lax.rem(q, 2)], out_hbm.at[q, me_r], sc_sem.at[lax.rem(q, 2), k - 1], rc_sem.at[q, k - 1],
                                            device_id={"r": to}, device_id_type=MESH)

    def own_copy(q):
        return pltpu.make_async_copy(sc.at[lax.rem(q, 2)], out_hbm.at[q, me_r], own_sem.at[lax.rem(q, 2)])

    def pack(q):
        to = lax.rem(q, 2)
        @pl.when(q >= 2)
        def _():
            for k in range(1, NS):
                a_copy(q - 2, k).wait_send()
        for s in range(NS):
            for j in range(NS):
                for b in range(6):
                    if b < 2:
                        v = accg[160 * s + 80 * b:160 * s + 80 * b + 80, 128 * j:128 * j + 128]
                    elif b < 4:
                        v = accu[160 * s + 80 * (b - 2):160 * s + 80 * (b - 2) + 80, 128 * j:128 * j + 128]
                    else:
                        v = accd[160 * j + 80 * (b - 4):160 * j + 80 * (b - 4) + 80, 128 * s:128 * s + 128]
                    at = 80 * (b % 3)
                    sa[to, s, 2 * j + b // 3, at:at + 80, :] = v.astype(BF)
        for k in range(1, NS):
            a_copy(q, k).start()

    def a_load(q):
        for k in range(1, NS):
            a_copy(q, k).wait_recv()
        pltpu.make_async_copy(ra_hbm.at[q], va, l_sem.at[0]).start()

    def a_add(q):
        to = lax.rem(q, 2)
        pltpu.make_async_copy(ra_hbm.at[q], va, l_sem.at[0]).wait()
        @pl.when(q >= 2)
        def _():
            for k in range(1, NG):
                b_copy(q - 2, k).wait_send()
        @pl.loop(0, NG)
        def _(p):
            total = sa[to, me_s, p].astype(F32)
            for k in range(NS - 1):
                total += va[k, p].astype(F32)
            sb[to, p] = total.astype(BF)
        for k in range(1, NG):
            b_copy(q, k).start()

    def b_load(q):
        for k in range(1, NG):
            b_copy(q, k).wait_recv()
        pltpu.make_async_copy(rb_hbm.at[q], vb, l_sem.at[1]).start()

    def b_add(q):
        to = lax.rem(q, 2)
        pltpu.make_async_copy(rb_hbm.at[q], vb, l_sem.at[1]).wait()
        @pl.when(q >= 2)
        def _():
            for k in range(1, NG):
                c_copy(q - 2, k).wait_send()
            own_copy(q - 2).wait()
        total = sb[to, me_r].astype(F32)
        for k in range(NG - 1):
            total += vb[k].astype(F32)
        sc[to] = total.astype(BF)
        own_copy(q).start()
        for k in range(1, NG):
            c_copy(q, k).start()

    whole_dy = pltpu.make_async_copy(dy_hbm, dy_s, l_sem.at[2])

    @pl.when((p == 0) & (r == 0))
    def _():
        barrier = pltpu.get_barrier_semaphore()
        for k in range(1, NS):
            pl.semaphore_signal(barrier, inc=1, device_id={"s": lax.rem(me_s + k, NS)}, device_id_type=MESH)
        for k in range(1, NG):
            pl.semaphore_signal(barrier, inc=1, device_id={"r": lax.rem(me_r + k, NG)}, device_id_type=MESH)
        pl.semaphore_wait(barrier, NS + NG - 2)
        for g in range(3):
            gather_send(g, 0)
            gather_send(g, 1)
        whole_dy.start()
        relay(0)
        gather_wait(in_sem, 0, 1)
        gather_wait(in_sem, 0, 2)
        fetch(0)

    @pl.when((r == 1) & (p < Q - 3))
    def _():
        gather_send(p + 3, 0)
        gather_send(p + 3, 1)

    @pl.when((r == 5) & (p < Q - 1))
    def _():
        relay(p + 1)

    @pl.when((r == 7) & (p < Q - 1))
    def _():
        gather_wait(in_sem, p + 1, 1)
        gather_wait(in_sem, p + 1, 2)

    @pl.when((r == 7) & (p < 3 * F - 1))
    def _():
        fetch(p + 1)

    @pl.when(r == 0)
    def _():
        fetched(p)

    @pl.when((r == 0) & (phase >= 1))
    def _():
        accg[...] = jnp.zeros_like(accg)
        accu[...] = jnp.zeros_like(accu)
        accd[...] = jnp.zeros_like(accd)

    def keep(wide):
        a = (wide * scale_of(wide)).astype(BF)
        a_s[rows] = a
        at_s[:, rows] = a.T

    @pl.when(f == 0)
    def _():
        da_s[rows] = jnp.zeros((R, D), F32)

    @pl.when((f == 0) & (phase != 1))
    def _():
        keep(x_ref[...].astype(F32))

    @pl.when((p == F) & (r == 0))
    def _():
        whole_dy.wait()
        h_out(NR - 2).wait()
        h_out(NR - 1).wait()

    @pl.when(p == F)
    def _():
        dyt_s[:, rows] = dy_s[rows].T

    @pl.when(phase == 0)
    def _():
        a = a_s[rows]
        gate = dot(a, wg_s[slot])
        up = dot(a, wu_s[slot])
        da_s[rows] += dot((gate * sigmoid(gate) * up).astype(BF), wd_s[slot])

    @pl.when(p == F - 1)
    def _():
        @pl.when(r >= 2)
        def _():
            h_out(r - 2).wait()
        h1 = (x_ref[...].astype(F32) + da_s[rows].astype(BF).astype(F32)).astype(BF)
        h_s[lax.rem(r, 2)] = h1
        keep(h1.astype(F32))
        h_out(r).start()

    @pl.when(phase >= 1)
    def _():
        a = a_s[rows]
        wg, wu, wd = wg_s[slot], wu_s[slot], wd_s[slot]
        gate = dot(a, wg)
        up = dot(a, wu)
        by_prod = dot_nt(dy_s[rows], wd).astype(BF).astype(F32)
        sig = sigmoid(gate)
        silu = gate * sig
        prod = (silu * up).astype(BF)
        by_up = (by_prod * silu).astype(BF)
        by_gate = (by_prod * up * (sig + silu * (1.0 - sig))).astype(BF)
        accd[...] += dot(dyt_s[:, rows], prod)
        at = at_s[:, rows]
        accg[...] += dot(at, by_gate)
        accu[...] += dot(at, by_up)
        da_s[rows] += dot_nt(by_gate, wg) + dot_nt(by_up, wu)

    def back(h):
        wide = h.astype(F32)
        scale = scale_of(wide)
        unit = wide * scale
        da = da_s[rows]
        by_wide = scale * (da - unit * jnp.mean(da * unit, -1, keepdims=True))
        return (dy_s[rows].astype(F32) + by_wide.astype(BF).astype(F32)).astype(BF)

    @pl.when((p == 2 * F - 2) & (r == NR - 1))
    def _():
        h_in(0).start()

    @pl.when(p == 2 * F - 1)
    def _():
        h_in(r).wait()
        @pl.when(r < NR - 1)
        def _():
            h_in(r + 1).start()
        by_h = back(h_s[lax.rem(r, 2)])
        dy_s[rows] = by_h
        dyt_s[:, rows] = by_h.T

    @pl.when(p == 3 * F - 1)
    def _():
        dx_ref[...] = back(x_ref[...])

    @pl.when((r == 6) & (q >= 1))
    def _():
        a_load(q - 1)

    @pl.when((r == 7) & (q >= 1))
    def _():
        a_add(q - 1)

    @pl.when((r == 7) & (q >= 0))
    def _():
        pack(q)

    @pl.when((r == 3) & (q >= 2))
    def _():
        b_load(q - 2)

    @pl.when((r == 4) & (q >= 2))
    def _():
        b_add(q - 2)

    @pl.when((q == Q - 1) & (r == NR - 1))
    def _():
        b_load(Q - 2)
        b_add(Q - 2)
        a_load(Q - 1)
        a_add(Q - 1)
        b_load(Q - 1)
        b_add(Q - 1)
        for last in (Q - 2, Q - 1):
            for k in range(1, NS):
                a_copy(last, k).wait_send()
            for k in range(1, NG):
                b_copy(last, k).wait_send()
                c_copy(last, k).wait_send()
            own_copy(last).wait()
        @pl.loop(0, Q)
        def _(each):
            for k in range(1, NG):
                c_copy(each, k).wait_recv()
            for way in range(3):
                gather_wait(out_sem, each, way)


def both_passes(x, dy, weights):
    hbm = pl.BlockSpec(memory_space=pl.ANY)

    def tile(phase, f, r):
        return jnp.where((phase != 1) & ((f == 0) | (f == F - 1)), r, NR - 1), 0

    def last(phase, f, r):
        return jnp.where((phase == 2) & (f == F - 1), r, 0), 0

    dma = pltpu.SemaphoreType.DMA
    dx, out, *_ = pl.pallas_call(
        kernel,
        grid=(3, F, NR),
        in_specs=[pl.BlockSpec((R, D), tile)] + [hbm] * 4,
        out_specs=[pl.BlockSpec((R, D), last)] + [hbm] * 7,
        out_shape=[
            jax.ShapeDtypeStruct((T, D), BF),
            jax.ShapeDtypeStruct((Q, NG, PIECE, 128), BF),
            jax.ShapeDtypeStruct((Q, NS - 1, NG, PIECE, 128), BF),
            jax.ShapeDtypeStruct((Q, NG - 1, PIECE, 128), BF),
            jax.ShapeDtypeStruct((T, D), BF),
            jax.ShapeDtypeStruct((Q, NS, 160, C), BF),
            jax.ShapeDtypeStruct((Q, NS, 160, C), BF),
            jax.ShapeDtypeStruct((Q, NS, 128, D), BF),
        ],
        scratch_shapes=[
            pltpu.VMEM((T, D), BF), pltpu.VMEM((D, T), BF), pltpu.VMEM((T, D), BF), pltpu.VMEM((D, T), BF),
            pltpu.VMEM((T, D), F32),
            pltpu.VMEM((D, C), F32), pltpu.VMEM((D, C), F32), pltpu.VMEM((D, C), F32),
            pltpu.VMEM((2, D, C), BF), pltpu.VMEM((2, D, C), BF), pltpu.VMEM((2, C, D), BF),
            pltpu.VMEM((2, NS, NG, PIECE, 128), BF), pltpu.VMEM((2, NG, PIECE, 128), BF), pltpu.VMEM((2, PIECE, 128), BF),
            pltpu.VMEM((NS - 1, NG, PIECE, 128), BF), pltpu.VMEM((NG - 1, PIECE, 128), BF), pltpu.VMEM((2, R, D), BF),
            dma((2, 3)), dma((3,)), dma((2, NS - 1)), dma((Q, NS - 1)), dma((2, NG - 1)), dma((Q, NG - 1)),
            dma((2, NG - 1)), dma((Q, NG - 1)), dma((2,)), dma((2,)), dma((3, Q)), dma((3, Q)),
        ],
        compiler_params=pltpu.CompilerParams(
            dimension_semantics=("arbitrary",) * 3, vmem_limit_bytes=63 * MB, collective_id=1, has_side_effects=True),
        cost_estimate=pl.CostEstimate(flops=38 * T * D * FF, bytes_accessed=100 * MB, transcendentals=0),
        name="both_passes",
    )(x, dy, *weights)
    return dx, out


def solution(mesh):
    def step(x, dy, *weights):
        dx, out = both_passes(x[0], dy[0], weights)
        sums = out.reshape(2, F, NS, 480, 128)[::-1]
        cut = lambda i: sums[:, :, :, 160 * i:160 * (i + 1)]
        wide = lambda v: v.transpose(0, 3, 2, 1, 4).reshape(2, 160, FF)
        down = cut(2).transpose(0, 1, 4, 2, 3).reshape(2, D, D)
        return dx[None], wide(cut(0)), wide(cut(1)), down

    states, cut = P(("rep", "r", "s"), None, None), P(None, "s", None)
    return jax.shard_map(
        step,
        mesh=mesh,
        in_specs=(states, states) + (cut,) * 3,
        out_specs=(states,) + (P("rep", "s", None),) * 3,
        check_vma=False,
    )
```

```python
import functools

import jax
import jax.numpy as jnp
from jax import lax
from jax.experimental import pallas as pl
from jax.experimental.pallas import tpu as pltpu
from jax.sharding import PartitionSpec as P

T, D, FF = 4096, 640, 2560
R = 512
NR = T // R
F, C = 5, 512
Q = 2 * F
NS, NG = 4, 8
BLOCK, PIECE = 1920, 240
BF, F32 = jnp.bfloat16, jnp.float32
MB = 1 << 20
MESH = pl.DeviceIdType.MESH
NT = (((1,), (1,)), ((), ()))


def dot(a, b):
    return jnp.dot(a, b, preferred_element_type=F32)


def dot_nt(a, b):
    return lax.dot_general(a, b, NT, preferred_element_type=F32)


def sigmoid(v):
    return 1.0 / (1.0 + jnp.exp(-v))


def scale_of(wide):
    return lax.rsqrt(jnp.mean(wide * wide, -1, keepdims=True) + 1e-6)


def kernel(x_hbm, dy_hbm, wg_in, wu_in, wd_in,
           dx_hbm, out_g, out_u, out_d, r1_hbm, r2_hbm, rb_hbm, h1_hbm, by_hbm, gg, gu, gd,
           a_s, at_s, dy_s, dyt_s, da_s, accg, accu, accd, wg_s, wu_s, wd_s,
           sa, sx, sb, sc, scd, v1, v2, vb, x_s, h_s, by_s,
           w_sem, l_sem, s1_sem, r1_sem, s2_sem, r2_sem, sb_sem, rb_sem, sc_sem, rc_sem, own_sem, x_sem, h_sem, by_sem, out_sem, in_sem):
    phase, f, r = pl.program_id(0), pl.program_id(1), pl.program_id(2)
    p = phase * F + f
    q = p - F
    slot = lax.rem(p, 2)
    me_s, me_r = lax.axis_index("s"), lax.axis_index("r")
    across = lax.rem(me_s + 2, NS)
    beside = me_s + 1 - 2 * lax.rem(me_s, 2)
    rows = pl.ds(pl.multiple_of(r * R, R), R)
    now = f * NR + r
    turn = lax.rem(r, 2)

    def mine(g):
        layer, part = g // F, lax.rem(g, F)
        for j in range(NS):
            units = pl.ds(pl.multiple_of(640 * j + 128 * part, 128), 128)
            yield 0, wg_in.at[layer, :, units], j
            yield 1, wu_in.at[layer, :, units], j
        yield 2, wd_in.at[layer, pl.ds(pl.multiple_of(128 * part, 128), 128)], 0

    def gather_send(g, way):
        to = across if way == 0 else beside
        owner = across if way == 2 else me_s
        if way == 2:
            pieces = [(m.at[g, owner], m.at[g, owner]) for m in (gg, gu, gd)]
        else:
            pieces = []
            for matrix, ref, j in mine(g):
                pieces.append((ref, gd.at[g, owner] if matrix == 2 else (gg, gu)[matrix].at[g, owner, :, pl.ds(128 * j, 128)]))
        for src, dst in pieces:
            pltpu.make_async_remote_copy(src, dst, out_sem.at[way, g], in_sem.at[way, g],
                                         device_id={"s": to}, device_id_type=MESH).start()

    def gather_wait(sem, g, way):
        pltpu.make_async_copy(r2_hbm.at[0], r2_hbm.at[0], sem.at[way, g]).wait()

    def relay(g):
        gather_wait(in_sem, g, 0)
        gather_send(g, 2)

    def fetch(p):
        to = lax.rem(p, 2)
        g = jnp.where(p < Q, p, lax.rem(p, F))
        for matrix, ref, j in mine(g):
            if matrix == 2:
                dst = wd_s.at[to, pl.ds(pl.multiple_of(128 * me_s, 128), 128)]
            else:
                dst = (wg_s, wu_s)[matrix].at[to, pl.ds(pl.multiple_of(160 * me_s, 32), 160), pl.ds(128 * j, 128)]
            pltpu.make_async_copy(ref, dst, w_sem.at[to, matrix]).start()
        for k in range(1, NS):
            s = lax.rem(me_s + k, NS)
            here = pl.ds(pl.multiple_of(160 * s, 32), 160)
            pltpu.make_async_copy(gg.at[g, s], wg_s.at[to, here], w_sem.at[to, 0]).start()
            pltpu.make_async_copy(gu.at[g, s], wu_s.at[to, here], w_sem.at[to, 1]).start()
            pltpu.make_async_copy(gd.at[g, s], wd_s.at[to, pl.ds(pl.multiple_of(128 * s, 128), 128)], w_sem.at[to, 2]).start()

    def fetched(p):
        to = lax.rem(p, 2)
        for matrix, w in enumerate((wg_s, wu_s, wd_s)):
            pltpu.make_async_copy(w.at[to], w.at[to], w_sem.at[to, matrix]).wait()

    def h_out(r):
        return pltpu.make_async_copy(h_s.at[lax.rem(r, 2)], h1_hbm.at[pl.ds(pl.multiple_of(r * R, R), R)], h_sem.at[lax.rem(r, 2)])

    def h_in(r):
        return pltpu.make_async_copy(h1_hbm.at[pl.ds(pl.multiple_of(r * R, R), R)], h_s.at[lax.rem(r, 2)], h_sem.at[lax.rem(r, 2)])


    def x_in(r):
        return pltpu.make_async_copy(x_hbm.at[pl.ds(pl.multiple_of(r * R, R), R)], x_s.at[lax.rem(r, 2)], x_sem.at[lax.rem(r, 2)])

    def x_tile():
        @pl.when(r < NR - 1)
        def _():
            x_in(r + 1).start()
        x_in(r).wait()
        return x_s[turn]

    def dx_out(r):
        return pltpu.make_async_copy(h_s.at[lax.rem(r, 2)], dx_hbm.at[pl.ds(pl.multiple_of(r * R, R), R)], h_sem.at[lax.rem(r, 2)])

    def by_out(t):
        return pltpu.make_async_copy(by_s.at[lax.rem(t, 2)], by_hbm.at[t], by_sem.at[lax.rem(t, 2)])

    def by_in(t):
        return pltpu.make_async_copy(by_hbm.at[t], by_s.at[lax.rem(t, 2)], by_sem.at[lax.rem(t, 2)])

    def s1_copy(q, i):
        to = beside if i == 0 else lax.rem(beside + 2, NS)
        return pltpu.make_async_remote_copy(sa.at[lax.rem(q, 2), to], r1_hbm.at[q, i], s1_sem.at[lax.rem(q, 2), i], r1_sem.at[q, i],
                                            device_id={"s": beside}, device_id_type=MESH)

    def s2_copy(q):
        return pltpu.make_async_remote_copy(sx, r2_hbm.at[q], s2_sem.at[0], r2_sem.at[q], device_id={"s": across}, device_id_type=MESH)

    def b_copy(q, k):
        to = lax.rem(me_r + k, NG)
        return pltpu.make_async_remote_copy(sb.at[lax.rem(q, 2), to], rb_hbm.at[q, k - 1], sb_sem.at[lax.rem(q, 2), k - 1], rb_sem.at[q, k - 1],
                                            device_id={"r": to}, device_id_type=MESH)

    def places(q):
        to, layer, part = lax.rem(q, 2), 1 - q // F, lax.rem(q, F)
        units = pl.ds(pl.multiple_of(640 * (me_r // 2) + 128 * part, 128), 128)
        some = pl.ds(pl.multiple_of(80 * lax.rem(me_r, 2), 16), 80)
        yield sc.at[to, 0], out_g.at[layer, some, units]
        yield sc.at[to, 1], out_u.at[layer, some, units]
        yield scd.at[to], out_d.at[layer, pl.ds(pl.multiple_of(128 * part + 16 * me_r, 16), 16)]

    def c_send(q):
        to = lax.rem(q, 2)
        for src, dst in places(q):
            pltpu.make_async_copy(src, dst, own_sem.at[to]).start()
            for k in range(1, NG):
                pltpu.make_async_remote_copy(src, dst, sc_sem.at[to, k - 1], rc_sem.at[q, k - 1],
                                             device_id={"r": lax.rem(me_r + k, NG)}, device_id_type=MESH).start()

    def c_wait(sem):
        pltpu.make_async_copy(rb_hbm.at[0, 0], rb_hbm.at[0, 0], sem).wait()

    def c_sent(q):
        to = lax.rem(q, 2)
        c_wait(own_sem.at[to])
        for k in range(1, NG):
            c_wait(sc_sem.at[to, k - 1])

    def pack(q):
        to = lax.rem(q, 2)
        @pl.when(q >= 2)
        def _():
            s1_copy(q - 2, 0).wait_send()
            s1_copy(q - 2, 1).wait_send()
        for s in range(NS):
            for j in range(NS):
                for h in range(2):
                    at = 160 * (2 * j + h)
                    here = slice(160 * s + 80 * h, 160 * s + 80 * h + 80), slice(128 * j, 128 * j + 128)
                    sa[to, s, at:at + 80] = accg[here].astype(BF)
                    sa[to, s, at + 80:at + 160] = accu[here].astype(BF)
            sa[to, s, 1280:] = accd[:, 128 * s:128 * s + 128].astype(BF)
        s1_copy(q, 0).start()
        s1_copy(q, 1).start()

    def s1_load(q):
        s1_copy(q, 0).wait_recv()
        s1_copy(q, 1).wait_recv()
        pltpu.make_async_copy(r1_hbm.at[q], v1, l_sem.at[0]).start()

    def s1_add(q):
        pltpu.make_async_copy(r1_hbm.at[q], v1, l_sem.at[0]).wait()
        @pl.when(q >= 1)
        def _():
            s2_copy(q - 1).wait_send()
        @pl.loop(0, 8)
        def _(p):
            at = pl.ds(pl.multiple_of(240 * p, 16), 240)
            sx[at] = (sa[lax.rem(q, 2), across, at].astype(F32) + v1[1, at].astype(F32)).astype(BF)
        s2_copy(q).start()

    def s2_load(q):
        s2_copy(q).wait_recv()
        pltpu.make_async_copy(r2_hbm.at[q], v2, l_sem.at[1]).start()

    def s2_add(q):
        to = lax.rem(q, 2)
        pltpu.make_async_copy(r2_hbm.at[q], v2, l_sem.at[1]).wait()
        @pl.when(q >= 2)
        def _():
            for k in range(1, NG):
                b_copy(q - 2, k).wait_send()
        def total(at):
            return (sa[to, me_s, at].astype(F32) + v1[0, at].astype(F32) + v2[at].astype(F32)).astype(BF)
        @pl.loop(0, NG)
        def _(p):
            sb[to, p, :160] = total(pl.ds(pl.multiple_of(160 * p, 32), 160))
        down = total(pl.ds(1280, 640)).T
        for p in range(NG):
            for t in range(5):
                sb[to, p, 160 + 16 * t:176 + 16 * t] = down[16 * p:16 * p + 16, 128 * t:128 * t + 128]
        for k in range(1, NG):
            b_copy(q, k).start()

    def b_load(q):
        for k in range(1, NG):
            b_copy(q, k).wait_recv()
        pltpu.make_async_copy(rb_hbm.at[q], vb, l_sem.at[2]).start()

    def b_add(q):
        to = lax.rem(q, 2)
        pltpu.make_async_copy(rb_hbm.at[q], vb, l_sem.at[2]).wait()
        @pl.when(q >= 2)
        def _():
            c_sent(q - 2)
        total = sb[to, me_r].astype(F32)
        for k in range(NG - 1):
            total += vb[k].astype(F32)
        total = total.astype(BF)
        sc[to, 0] = total[:80]
        sc[to, 1] = total[80:160]
        for t in range(5):
            scd[to, :, 128 * t:128 * t + 128] = total[160 + 16 * t:176 + 16 * t]
        c_send(q)

    whole_dy = pltpu.make_async_copy(dy_hbm, dy_s, l_sem.at[3])

    def keep(wide, rows):
        a = (wide * scale_of(wide)).astype(BF)
        a_s[rows] = a
        at_s[:, rows] = a.T

    def begin():
        barrier = pltpu.get_barrier_semaphore()
        x_in(0).start()
        for k in range(1, NS):
            pl.semaphore_signal(barrier, inc=1, device_id={"s": lax.rem(me_s + k, NS)}, device_id_type=MESH)
        for k in range(1, NG):
            pl.semaphore_signal(barrier, inc=1, device_id={"r": lax.rem(me_r + k, NG)}, device_id_type=MESH)
        pl.semaphore_wait(barrier, NS + NG - 2)
        for g in range(3):
            gather_send(g, 0)
            gather_send(g, 1)

        @pl.loop(0, NR)
        def _(i):
            @pl.when(i < NR - 1)
            def _():
                x_in(i + 1).start()
            x_in(i).wait()
            here = pl.ds(pl.multiple_of(i * R, R), R)
            keep(x_s[lax.rem(i, 2)].astype(F32), here)
            da_s[i] = jnp.zeros((D, R), F32)

        whole_dy.start()
        relay(0)
        gather_wait(in_sem, 0, 1)
        gather_wait(in_sem, 0, 2)
        fetch(0)

    def clear():
        accg[...] = jnp.zeros_like(accg)
        accu[...] = jnp.zeros_like(accu)
        accd[...] = jnp.zeros_like(accd)

    def weights_of_next():
        @pl.when(p < Q - 1)
        def _():
            gather_wait(in_sem, p + 1, 1)
            gather_wait(in_sem, p + 1, 2)
        pl.when(p < 4 * F - 1)(lambda: fetch(p + 1))
        pl.when((p == F - 2) | (p == 2 * F - 1) | (p == 4 * F - 2))(lambda: x_in(0).start())

    def send_later():
        gather_send(p + 3, 0)
        gather_send(p + 3, 1)

    @pl.when(r == 0)
    def _():
        pl.when(p == 0)(begin)
        fetched(p)
        pl.when((q >= 0) & (q < Q))(clear)

    @pl.when(((r == 1) | (r == 4)) & (p < Q - 1))
    def _():
        pl.when((r == 1) & (p < Q - 3))(send_later)
        pl.when(r == 4)(lambda: relay(p + 1))

    @pl.when(r == 6)
    def _():
        weights_of_next()

    @pl.when((f == 0) & (phase > 0))
    def _():
        da_s[r] = jnp.zeros((D, R), F32)

        @pl.when(phase == 1)
        def _():
            @pl.when(r == 0)
            def _():
                whole_dy.wait()
                h_out(NR - 2).wait()
                h_out(NR - 1).wait()
            dyt_s[:, rows] = dy_s[rows].T

        @pl.when(phase == 2)
        def _():
            keep(x_tile().astype(F32), rows)

    @pl.when(phase == 0)
    def _():
        a = a_s[rows]
        gate = dot(a, wg_s[slot])
        up = dot(a, wu_s[slot])
        h = dot((gate * sigmoid(gate) * up).astype(BF), wd_s[slot])
        da_s[r, :R] += h[:, :C]
        for i in range(4):
            da_s[r, R:, 128 * i:128 * i + 128] += h[128 * i:128 * i + 128, C:]

    @pl.when(phase >= 2)
    def _():
        pl.when((phase == 2) & (now >= 2))(lambda: by_out(now - 2).wait())

        @pl.when(phase == 3)
        def _():
            @pl.when(now == 0)
            def _():
                by_out(F * NR - 2).wait()
                by_out(F * NR - 1).wait()
                by_in(0).start()
            @pl.when(now < F * NR - 1)
            def _():
                by_in(now + 1).start()
            by_in(now).wait()

    def main(whole):
        a = a_s[rows]
        wg, wu, wd = wg_s[slot], wu_s[slot], wd_s[slot]
        gate = dot(a, wg)
        up = dot(a, wu)
        by_prod = dot_nt(dy_s[rows], wd).astype(BF).astype(F32)
        sig = sigmoid(gate)
        silu = gate * sig
        prod = (silu * up).astype(BF)
        by_up = (by_prod * silu).astype(BF)
        by_gate = (by_prod * up * (sig + silu * (1.0 - sig))).astype(BF)
        accd[...] += dot(dyt_s[:, rows], prod)
        at = at_s[:, rows]
        accg[...] += dot(at, by_gate)
        accu[...] += dot(at, by_up)
        if whole:
            da_s[r] += dot_nt(wg, by_gate) + dot_nt(wu, by_up)
        else:
            by_s[turn, 0] = by_gate
            by_s[turn, 1] = by_up
            by_out(now).start()

    @pl.when(phase == 1)
    def _():
        main(True)

    @pl.when(phase == 2)
    def _():
        main(False)

    @pl.when(phase == 3)
    def _():
        da_s[r] += dot_nt(wg_s[slot], by_s[turn, 0]) + dot_nt(wu_s[slot], by_s[turn, 1])

    def back(h):
        wide = h.astype(F32)
        scale = scale_of(wide)
        unit = wide * scale
        da = da_s[r].T
        by_wide = scale * (da - unit * jnp.mean(da * unit, -1, keepdims=True))
        return (dy_s[rows].astype(F32) + by_wide.astype(BF).astype(F32)).astype(BF)

    @pl.when(f == F - 1)
    def _():
        @pl.when(phase == 0)
        def _():
            x = x_tile().astype(F32)
            pl.when(r >= 2)(lambda: h_out(r - 2).wait())
            rest = jnp.concatenate([da_s[r, R:, 128 * i:128 * i + 128] for i in range(4)], axis=0)
            h = jnp.concatenate([da_s[r, :R], rest], axis=1)
            h1 = (x + h.astype(BF).astype(F32)).astype(BF)
            h_s[turn] = h1
            keep(h1.astype(F32), rows)
            h_out(r).start()

        @pl.when(phase == 1)
        def _():
            pl.when(r == 0)(lambda: h_in(0).start())
            pl.when(r < NR - 1)(lambda: h_in(r + 1).start())
            h_in(r).wait()
            by_h = back(h_s[turn])
            dy_s[rows] = by_h
            dyt_s[:, rows] = by_h.T

        @pl.when(phase == 3)
        def _():
            x = x_tile()
            pl.when(r >= 2)(lambda: dx_out(r - 2).wait())
            h_s[turn] = back(x)
            dx_out(r).start()

    @pl.when((q >= 0) & (q <= Q))
    def _():
        @pl.when(r < 4)
        def _():
            pl.when((r == 1) & (q >= 1) & (q < Q))(lambda: s1_load(q - 1))
            pl.when((r == 2) & (q >= 1) & (q < Q))(lambda: s1_add(q - 1))
            pl.when((r == 3) & (q >= 2))(lambda: b_load(q - 2))

        @pl.when(r >= 4)
        def _():
            pl.when((r == 4) & (q >= 2))(lambda: b_add(q - 2))
            pl.when((r == 6) & (q >= 1) & (q < Q))(lambda: s2_load(q - 1))

            @pl.when((r == 7) & (q < Q))
            def _():
                pl.when(q >= 1)(lambda: s2_add(q - 1))
                pack(q)

    @pl.when(phase == 3)
    def _():
        pl.when(now == 2)(lambda: s1_load(Q - 1))
        pl.when(now == 3)(lambda: s1_add(Q - 1))
        pl.when(now == 15)(lambda: s2_load(Q - 1))
        pl.when(now == 16)(lambda: s2_add(Q - 1))
        pl.when(now == 28)(lambda: b_load(Q - 1))
        pl.when(now == 29)(lambda: b_add(Q - 1))

        @pl.when(now == F * NR - 1)
        def _():
            dx_out(NR - 2).wait()
            dx_out(NR - 1).wait()
            s2_copy(Q - 1).wait_send()
            for last in (Q - 2, Q - 1):
                s1_copy(last, 0).wait_send()
                s1_copy(last, 1).wait_send()
                for k in range(1, NG):
                    b_copy(last, k).wait_send()
                c_sent(last)
            @pl.loop(0, Q)
            def _(each):
                for k in range(1, NG):
                    c_wait(rc_sem.at[each, k - 1])
                for way in range(3):
                    gather_wait(out_sem, each, way)


def both_passes(x, dy, weights):
    hbm = pl.BlockSpec(memory_space=pl.ANY)

    dma = pltpu.SemaphoreType.DMA
    dx, g, u, d, *_ = pl.pallas_call(
        kernel,
        grid=(4, F, NR),
        in_specs=[hbm] * 5,
        out_specs=[hbm] * 12,
        out_shape=[
            jax.ShapeDtypeStruct((T, D), BF),
            jax.ShapeDtypeStruct((2, 160, FF), BF),
            jax.ShapeDtypeStruct((2, 160, FF), BF),
            jax.ShapeDtypeStruct((2, D, D), BF),
            jax.ShapeDtypeStruct((Q, 2, BLOCK, 128), BF),
            jax.ShapeDtypeStruct((Q, BLOCK, 128), BF),
            jax.ShapeDtypeStruct((Q, NG - 1, PIECE, 128), BF),
            jax.ShapeDtypeStruct((T, D), BF),
            jax.ShapeDtypeStruct((F * NR, 2, R, C), BF),
            jax.ShapeDtypeStruct((Q, NS, 160, C), BF),
            jax.ShapeDtypeStruct((Q, NS, 160, C), BF),
            jax.ShapeDtypeStruct((Q, NS, 128, D), BF),
        ],
        scratch_shapes=[
            pltpu.VMEM((T, D), BF), pltpu.VMEM((D, T), BF), pltpu.VMEM((T, D), BF), pltpu.VMEM((D, T), BF),
            pltpu.VMEM((NR, D, R), F32),
            pltpu.VMEM((D, C), F32), pltpu.VMEM((D, C), F32), pltpu.VMEM((D, C), F32),
            pltpu.VMEM((2, D, C), BF), pltpu.VMEM((2, D, C), BF), pltpu.VMEM((2, C, D), BF),
            pltpu.VMEM((2, NS, BLOCK, 128), BF), pltpu.VMEM((BLOCK, 128), BF), pltpu.VMEM((2, NG, PIECE, 128), BF),
            pltpu.VMEM((2, 2, 80, 128), BF), pltpu.VMEM((2, 16, D), BF),
            pltpu.VMEM((2, BLOCK, 128), BF), pltpu.VMEM((BLOCK, 128), BF), pltpu.VMEM((NG - 1, PIECE, 128), BF),
            pltpu.VMEM((2, R, D), BF), pltpu.VMEM((2, R, D), BF), pltpu.VMEM((2, 2, R, C), BF),
            dma((2, 3)), dma((4,)), dma((2, 2)), dma((Q, 2)), dma((1,)), dma((Q,)), dma((2, NG - 1)), dma((Q, NG - 1)),
            dma((2, NG - 1)), dma((Q, NG - 1)), dma((2,)), dma((2,)), dma((2,)), dma((2,)), dma((3, Q)), dma((3, Q)),
        ],
        compiler_params=pltpu.CompilerParams(
            dimension_semantics=("arbitrary",) * 3, vmem_limit_bytes=63 * MB, collective_id=1, has_side_effects=True),
        cost_estimate=pl.CostEstimate(flops=38 * T * D * FF, bytes_accessed=100 * MB, transcendentals=0),
        name="both_passes",
    )(x, dy, *weights)
    return dx[None], g, u, d


def solution(mesh):
    def step(x, dy, *weights):
        return both_passes(x[0], dy[0], weights)

    states, cut = P(("rep", "r", "s"), None, None), P(None, "s", None)
    return jax.shard_map(
        step,
        mesh=mesh,
        in_specs=(states, states) + (cut,) * 3,
        out_specs=(states,) + (P("rep", "s", None),) * 3,
        check_vma=False,
    )
```
